256 devices in a mesh: loop: 256 (over z, y, x, core).
Axes of the slice: x: 4, y: 4, z: 8, core: 2. Of those that a mesh axis runs over, the one named last changes fastest.
Arguments:
- signal: float32 [256, 8192, 256], P('loop'), may hold values from -8 to 8, as said below
- tap_gain: float32 [3, 256], replicated, may hold values from 0.3 to 1.2
Outputs:
- filtered: float32 [256, 8192, 256], P('loop')
The draws below stay inside these ranges and needn't reach their ends.
Inputs may be any that keep to these rules, and one draw needn't show every extreme that they name: signal holds numbers from -8 to 8.
All inputs are finite; a program needn't handle non-finite values.
Results may differ from the reference program's by a relative error of at most 0.0003.
Values sent between devices are 32-bit elements.
No kernel may reach another device: no remote copies, remote signals or barrier semaphores. Data moves between devices by JAX's collectives and lax.ppermute only.
A program may use at most 64 MiB of HBM per device.

```python
import jax
import jax.numpy as jnp

STEPS_DEV = 8192
CHANNELS = 256
SEGMENTS = 256


def draw_signal(key, part):
    keys = jax.random.split(key, 2)
    loud = jnp.exp(jax.random.uniform(keys[0], (SEGMENTS, 1, CHANNELS), jnp.float32, -1.2, 1.2))
    noise = jax.random.normal(keys[1], (SEGMENTS, STEPS_DEV, CHANNELS), jnp.float32)
    return jnp.clip(loud * noise, -8.0, 8.0)


def setup_inputs(seed: int = 0) -> dict:
    seeds = jax.random.split(jax.random.key(seed), 3)
    return {
        "signal": draw_signal(jax.random.fold_in(seeds[2], 71), 0),
        "tap_gain": jnp.clip(jax.random.uniform(seeds[1], (3, CHANNELS), jnp.float32, 0.3, 1.2), 0.3, 1.2),
    }


def reference(signal, tap_gain):
    wide_in = signal.astype(jnp.float32)
    mixed = tap_gain[0] * wide_in + tap_gain[1] * jnp.roll(wide_in, 33, axis=0) + tap_gain[2] * jnp.roll(wide_in, 127, axis=0)
    filtered = jnp.tanh(mixed).astype(jnp.float32)
    return filtered
```

```python
import functools

import jax
import jax.numpy as jnp
from jax import lax
from jax.experimental import pallas as pl
from jax.experimental.pallas import tpu as pltpu
from jax.sharding import PartitionSpec as P


UP = (880, 880, 880, 880)
DOWN = (1168, 1168, 1168, 1168)
STEP = {880: 440, 1168: 584}


def passed_along(value, axis, steps):
    count = lax.axis_size(axis)
    pairs = [(source, (source + steps) % count) for source in range(count)]
    return lax.ppermute(value, axis, pairs)


def mix_kernel(start, rows, step, gain, own, copy_1, copy_2, *refs):
    out = refs[-1]

    def tile(own, copy_1, copy_2, out):
        mixed = gain[0:1] * own[0] + gain[1:2] * copy_1[0] + gain[2:3] * copy_2[0]
        out[0] = jnp.tanh(mixed)

    spec = pl.BlockSpec((1, step, own.shape[2]), lambda i: (0, i, 0))
    pltpu.emit_pipeline(
        tile, grid=(rows // step,), in_specs=[spec] * 3, out_specs=[spec]
    )(own, copy_1, copy_2, out.at[:, pl.ds(start, rows), :])


def mix(filtered, shape, start, own, copy_1, copy_2, gain):
    rows = own.shape[1]
    anywhere = pl.BlockSpec(memory_space=pl.ANY)
    args = (gain, own, copy_1, copy_2) + (() if filtered is None else (filtered,))
    size = own.size
    return pl.pallas_call(
        functools.partial(mix_kernel, start, rows, STEP[rows]),
        out_shape=jax.ShapeDtypeStruct(shape, own.dtype),
        in_specs=[pl.BlockSpec(memory_space=pltpu.VMEM)] + [anywhere] * (len(args) - 1),
        out_specs=pl.BlockSpec(memory_space=pltpu.HBM),
        input_output_aliases={} if filtered is None else {4: 0},
        cost_estimate=pl.CostEstimate(flops=6 * size, bytes_accessed=16 * size, transcendentals=size),
    )(*args)


def body(signal, tap_gain):
    starts, at = [], 0
    for size in UP + DOWN:
        starts.append(at)
        at += size
    assert at == signal.shape[1]
    own = [lax.slice_in_dim(signal, s, s + n, axis=1) for s, n in zip(starts, UP + DOWN)]
    n = len(UP)
    near = [passed_along(v, "loop", 33) for v in own]
    far = [passed_along(near[i], "loop", 94) for i in range(n)]
    for i in range(n, len(own)):
        half_way = passed_along(own[i], "loop", -96)
        far.append(passed_along(half_way, "loop", -33))
    filtered = None
    order = []
    for i in range(n):
        order += [i, n + i]
    for i in order:
        filtered = mix(filtered, signal.shape, starts[i], own[i], near[i], far[i], tap_gain)
    return filtered


def solution(mesh):
    return jax.shard_map(
        body,
        mesh=mesh,
        in_specs=(P("loop", None, None), P()),
        out_specs=P("loop", None, None),
        check_vma=False,
    )
```

```python
import functools

import jax
import jax.numpy as jnp
from jax import lax
from jax.experimental import pallas as pl
from jax.experimental.pallas import tpu as pltpu
from jax.sharding import PartitionSpec as P


AXIS, COUNT, PLANE = "loop", 256, 32
UP = ((960, -1), (960, -1), (960, -1), (624, -1))
DOWN = ((800, None, 0), (800, 3, 2), (800, 9, -2), (800, -7, 8), (800, 11, -8), (688, -5, 10))


def stop(source, planes, turn):
    plane, place = divmod(source, PLANE)
    return (plane + planes) * PLANE % COUNT + (place + turn) % PLANE


def send(value, begin, end):
    pairs = [(begin(s), end(s)) for s in range(COUNT)]
    return lax.ppermute(value, AXIS, pairs)


def mix_kernel(start, rows, step, gain, own, copy_1, copy_2, *refs):
    out = refs[-1]

    def tile(own, copy_1, copy_2, out):
        mixed = gain[0:1] * own[0] + gain[1:2] * copy_1[0] + gain[2:3] * copy_2[0]
        out[0] = jnp.tanh(mixed)

    spec = pl.BlockSpec((1, step, own.shape[2]), lambda i: (0, i, 0))
    pltpu.emit_pipeline(
        tile, grid=(rows // step,), in_specs=[spec] * 3, out_specs=[spec]
    )(own, copy_1, copy_2, out.at[:, pl.ds(start, rows), :])


def mix(filtered, shape, start, own, copy_1, copy_2, gain):
    rows = own.shape[1]
    anywhere = pl.BlockSpec(memory_space=pl.ANY)
    args = (gain, own, copy_1, copy_2) + (() if filtered is None else (filtered,))
    size = own.size
    return pl.pallas_call(
        functools.partial(mix_kernel, start, rows, rows // 2),
        out_shape=jax.ShapeDtypeStruct(shape, own.dtype),
        in_specs=[pl.BlockSpec(memory_space=pltpu.VMEM)] + [anywhere] * (len(args) - 1),
        out_specs=pl.BlockSpec(memory_space=pltpu.HBM),
        input_output_aliases={} if filtered is None else {4: 0},
        cost_estimate=pl.CostEstimate(flops=6 * size, bytes_accessed=16 * size, transcendentals=size),
    )(*args)


def body(signal, tap_gain):
    here = lambda s: s
    near_home = lambda s: (s + 33) % COUNT
    far_home = lambda s: (s + 127) % COUNT
    sizes = [piece[0] for piece in UP + DOWN]
    starts = [sum(sizes[:i]) for i in range(len(sizes))]
    assert sum(sizes) == signal.shape[1]
    own = [lax.slice_in_dim(signal, s, s + n, axis=1) for s, n in zip(starts, sizes)]
    near, far = [], []
    for i, (_, turn, *down) in enumerate(UP + DOWN):
        if turn is None:
            near.append(send(own[i], here, near_home))
        else:
            first = functools.partial(stop, planes=1, turn=turn)
            relay = send(own[i], here, first)
            near.append(send(relay, first, near_home))
        if down:
            first = functools.partial(stop, planes=-3, turn=down[0])
            relay = send(own[i], here, first)
            far.append(send(relay, first, far_home))
        else:
            far.append(send(relay, first, far_home))
    filtered = None
    for i in MIX_ORDER:
        filtered = mix(filtered, signal.shape, starts[i], own[i], near[i], far[i], tap_gain)
    return filtered


MIX_ORDER = [0, 4, 1, 5, 6, 2, 7, 8, 3, 9]


def solution(mesh):
    return jax.shard_map(
        body,
        mesh=mesh,
        in_specs=(P(AXIS, None, None), P()),
        out_specs=P(AXIS, None, None),
        check_vma=False,
    )
```

```python
import functools

import jax
import jax.numpy as jnp
from jax import lax
from jax.experimental import pallas as pl
from jax.experimental.pallas import tpu as pltpu
from jax.sharding import PartitionSpec as P


AXIS, COUNT, PLANE = "loop", 256, 32
UP = ((672, 1), (960, None), (960, 1), (960, 1))
DOWN = ((640, -2, 0), (800, 3, -1), (800, 1, -3), (800, 1, 2), (800, 1, 0), (800, 1, -1))


def stop(source, planes, turn):
    plane, place = divmod(source, PLANE)
    return (plane + planes) * PLANE % COUNT + (place + turn) % PLANE


def send(value, begin, end):
    pairs = [(begin(s), end(s)) for s in range(COUNT)]
    return lax.ppermute(value, AXIS, pairs)


def mix_kernel(start, rows, tiles, gain, own, copy_1, copy_2, *refs):
    out, tile, sems = refs[-3:]
    step = rows // tiles
    copies = []
    for i in range(tiles):
        part = pl.ds(i * step, step)
        mixed = gain[0:1] * own[0, part] + gain[1:2] * copy_1[0, part] + gain[2:3] * copy_2[0, part]
        tile[part] = jnp.tanh(mixed)
        copies.append(pltpu.make_async_copy(tile.at[part], out.at[0, pl.ds(start + i * step, step)], sems.at[i]))
        copies[-1].start()
    for copy in copies:
        copy.wait()


def mix(filtered, shape, start, own, copy_1, copy_2, gain):
    rows = own.shape[1]
    args = (gain, own, copy_1, copy_2) + (() if filtered is None else (filtered,))
    size = own.size
    return pl.pallas_call(
        functools.partial(mix_kernel, start, rows, TILES),
        out_shape=jax.ShapeDtypeStruct(shape, own.dtype),
        in_specs=[pl.BlockSpec(memory_space=pltpu.VMEM)] * 4
        + [pl.BlockSpec(memory_space=pltpu.HBM)] * (len(args) - 4),
        out_specs=pl.BlockSpec(memory_space=pltpu.HBM),
        scratch_shapes=[pltpu.VMEM((rows, shape[2]), own.dtype), pltpu.SemaphoreType.DMA((TILES,))],
        input_output_aliases={} if filtered is None else {4: 0},
        compiler_params=pltpu.CompilerParams(vmem_limit_bytes=8 << 20),
        cost_estimate=pl.CostEstimate(flops=6 * size, bytes_accessed=16 * size, transcendentals=size),
    )(*args)


TILES = 4


def body(signal, tap_gain):
    here = lambda s: s
    near_home = lambda s: (s + 33) % COUNT
    far_home = lambda s: (s + 127) % COUNT
    sizes = [piece[0] for piece in UP + DOWN]
    starts = [sum(sizes[:i]) for i in range(len(sizes))]
    assert sum(sizes) == signal.shape[1]
    own = [lax.slice_in_dim(signal, s, s + n, axis=1) for s, n in zip(starts, sizes)]
    near, far = [], []
    for i, (_, turn, *down) in enumerate(UP + DOWN):
        first = near_home if turn is None else functools.partial(stop, planes=1, turn=turn)
        relay = send(own[i], here, first)
        near.append(relay if turn is None else send(relay, first, near_home))
        if down:
            first = functools.partial(stop, planes=-3, turn=down[0])
            relay = send(own[i], here, first)
            far.append(send(relay, first, far_home))
        else:
            far.append(send(relay, first, far_home))
    filtered = None
    for i in MIX_ORDER:
        filtered = mix(filtered, signal.shape, starts[i], own[i], near[i], far[i], tap_gain)
    return filtered


MIX_ORDER = [4, 5, 0, 1, 6, 2, 7, 8, 3, 9]


def solution(mesh):
    return jax.shard_map(
        body,
        mesh=mesh,
        in_specs=(P(AXIS, None, None), P()),
        out_specs=P(AXIS, None, None),
        check_vma=False,
    )
```
